256 devices in a mesh: gz: 8 (over z), gx: 4 (over x), gy: 8 (over y, core).
Axes of the slice: x: 4, y: 4, z: 8, core: 2. Of those that a mesh axis runs over, the one named last changes fastest.
Arguments:
- density: float32 [256, 1024, 1024], P('gz', 'gy', 'gx'), may hold values from 0 to 1
- mask: int32 [32, 128, 128], P('gz', 'gy', 'gx'), may hold values from 0 to 3
Outputs:
- filtered: float32 [256, 1024, 1024], P(('gz', 'gx'), 'gy')
- projected: float32 [256, 1024, 1024], P(('gz', 'gx'), 'gy')
The draws below stay inside these ranges and needn't reach their ends.
Inputs may be any that keep to these rules, and one draw needn't show every extreme that they name: `mask`: code 0 marks a void block, 1 a solid block, 2 and 3 design blocks.
All inputs are finite; a program needn't handle non-finite values.
Results may differ from the reference program's by a relative error of at most 0.0003.
Values sent between devices are 32-bit elements; how exact they have to be, the bound alone decides.
No kernel may reach another device: no remote copies, remote signals or barrier semaphores. Data moves between devices by JAX's collectives and lax.ppermute only.
A program may use at most 128 MiB of HBM per device.

```python
import jax
import jax.numpy as jnp
from jax import lax

RADIUS = 6
CELLS = 8
NX = 1024
NY = 1024
NZ = 256


def set_ends(drawn, rng, smallest, high):
    dims = drawn.shape
    spot = [jax.random.randint(jax.random.fold_in(rng, axis), (), 0, dims[axis]) for axis in range(len(dims))]
    drawn = drawn.at[tuple(spot)].set(smallest)
    longest = dims.index(max(dims))
    spot[longest] = (spot[longest] + 1) % dims[longest]
    return drawn.at[tuple(spot)].set(high)


def steps_of(stream_key, shape, split, low, high):
    level = 1.0
    for dim, parts in split:
        steps = jax.random.uniform(jax.random.fold_in(jax.random.fold_in(stream_key, 6), dim), (parts,), jnp.float32, low / len(split), high / len(split))
        level = level * jnp.repeat(jnp.exp(steps), shape[dim] // parts).reshape((-1,) + (1,) * (len(shape) - 1 - dim))
    return level


def setup_inputs(seed: int = 0) -> dict:
    splits = jax.random.split(jax.random.key(seed), 3)
    return {
        "density": jnp.clip(1.0 * jax.random.uniform(splits[0], (NZ, NY, NX), jnp.float32) ** steps_of(splits[0], (NZ, NY, NX), ((0, 8), (1, 8), (2, 4)), -0.2, 0.2), 0.0, 1.0),
        "mask": set_ends(jax.random.randint(splits[1], (NZ // CELLS, NY // CELLS, NX // CELLS), 0, 4), jax.random.fold_in(splits[1], 1), 0, 3).astype(jnp.int32),
    }


sharpness = 8.0
threshold = 0.5


def smooth_axis(values, axis_index, count):
    widths = [(RADIUS, RADIUS) if position == axis_index else (0, 0) for position in range(values.ndim)]
    padded = jnp.pad(values, widths)
    result = jnp.zeros_like(values)
    for offset in range(-RADIUS, RADIUS + 1):
        window = lax.slice_in_dim(padded, RADIUS + offset, RADIUS + offset + count, axis=axis_index)
        result = result + float(RADIUS + 1 - abs(offset)) * window
    return result


def weight_count(count):
    return smooth_axis(jnp.ones((count,), jnp.float32), 0, count)


def reference(density, mask):
    def one_plane(item):
        plane, level = item
        block_row = mask[level // CELLS]
        design_code = jnp.repeat(jnp.repeat(block_row, CELLS, 0), CELLS, 1)
        physical = jnp.where(design_code == 0, 0.0, jnp.where(design_code == 1, 1.0, plane))
        return smooth_axis(smooth_axis(physical, 1, NX), 0, NY)

    levels = jnp.arange(NZ, dtype=jnp.int32)
    flat = lax.map(one_plane, (density, levels))
    summed = smooth_axis(flat, 0, NZ)
    counts = weight_count(NZ)[:, None, None] * weight_count(NY)[None, :, None] * weight_count(NX)[None, None, :]
    filtered = summed / counts
    top = jnp.tanh(sharpness * threshold)
    projected = (top + jnp.tanh(sharpness * (filtered - threshold))) / (top + jnp.tanh(sharpness * (1.0 - threshold)))
    return filtered, projected
```

```python
import functools

import jax
import jax.numpy as jnp
from jax import lax
from jax.experimental import pallas as pl
from jax.experimental.pallas import tpu as pltpu
from jax.sharding import PartitionSpec as P


RADIUS = 6
CELLS = 8
EDGE = 8
BOX = RADIUS + 1

sharpness = 8.0
threshold = 0.5


STAGES = (2, 2, 4)


def first_of(stage):
    return sum(STAGES[:stage])


def plane_offset(stage, quarter):
    ascending = first_of(stage)
    descending = sum(STAGES) - ascending - STAGES[stage]
    return jnp.where(quarter == 0, descending, ascending)


def hat(shape, shift):
    out_index = lax.broadcasted_iota(jnp.int32, shape, 0)
    in_index = lax.broadcasted_iota(jnp.int32, shape, 1)
    distance = jnp.abs(in_index + shift - out_index)
    return jnp.maximum(BOX - distance, 0)


def two_parts(values):
    high = values.astype(jnp.bfloat16)
    low = (values - high.astype(jnp.float32)).astype(jnp.bfloat16)
    return high, low


def along_rows(kernel, values):
    high, low = two_parts(values)
    return jnp.dot(kernel, high, preferred_element_type=jnp.float32) + jnp.dot(
        kernel, low, preferred_element_type=jnp.float32
    )


def vmem(count):
    return [pl.BlockSpec(memory_space=pltpu.VMEM)] * count


def params(mib):
    return pltpu.CompilerParams(vmem_limit_bytes=mib * 1024 * 1024)


def cost(flops):
    return pl.CostEstimate(flops=flops, bytes_accessed=8 * 1024 * 1024, transcendentals=0)


def section_kernel(density, mask, conv, first_rows, last_rows, *rest):
    sends, codes = rest[:4], rest[4]
    planes, rows, columns = density.shape
    blocks = rows // CELLS
    table = mask[...].reshape(planes // CELLS * blocks, columns // CELLS)
    spread = (
        lax.broadcasted_iota(jnp.int32, (columns // CELLS, columns), 1) // CELLS
        == lax.broadcasted_iota(jnp.int32, (columns // CELLS, columns), 0)
    )
    codes[...] = jnp.dot(
        table.astype(jnp.float32).astype(jnp.bfloat16),
        spread.astype(jnp.float32).astype(jnp.bfloat16),
        preferred_element_type=jnp.float32,
    )

    def tile(i, carry):
        row = pl.ds(pl.multiple_of(i * CELLS, CELLS), CELLS)
        values, boxes = [], []
        box = total = None
        for z in range(planes + 2 * RADIUS):
            if z < planes:
                if z % CELLS == 0:
                    code = jnp.broadcast_to(
                        codes[pl.ds(z // CELLS * blocks + i, 1), :], (CELLS, columns)
                    )
                    void, solid = code < 0.5, code < 1.5
                value = jnp.where(void, 0.0, jnp.where(solid, 1.0, density[z, row, :]))
                values.append(value)
                box = value if box is None else box + value
            if z < planes + RADIUS:
                if z >= BOX:
                    box = box - values[z - BOX]
                boxes.append(box)
                total = box if total is None else total + box
            if z >= BOX:
                total = total - boxes[z - BOX]
            conv[z, row, :] = total
        return carry

    lax.fori_loop(0, blocks, tile, 0)
    first_rows[...] = conv[:, :EDGE, :]
    last_rows[...] = conv[:, rows - EDGE :, :]
    kernel = hat((rows - 2 * EDGE, rows), -EDGE).astype(jnp.float32).astype(jnp.bfloat16)
    me = lax.axis_index("gx")
    for distance in range(4):
        quarter = lax.rem(me + distance, 4)
        base = RADIUS + 8 * quarter + plane_offset(0, quarter)
        for j in range(STAGES[0]):
            sends[distance][j] = along_rows(kernel, conv[base + j])


def section(density, mask):
    planes, rows, columns = density.shape
    span = planes + 2 * RADIUS
    f32 = functools.partial(jax.ShapeDtypeStruct, dtype=jnp.float32)
    return pl.pallas_call(
        section_kernel,
        out_shape=[
            f32((span, rows, columns)),
            f32((span, EDGE, columns)),
            f32((span, EDGE, columns)),
        ]
        + [f32((STAGES[0], rows - 2 * EDGE, columns))] * 4,
        in_specs=vmem(2),
        out_specs=vmem(7),
        scratch_shapes=[pltpu.VMEM((planes // CELLS * rows // CELLS, columns), jnp.float32)],
        compiler_params=params(24),
        cost_estimate=cost(40_000_000),
        name="section",
    )(density, mask)


def edges_kernel(conv, before, after, *outs):
    planes = conv.shape[0] - 2 * RADIUS
    rows = conv.shape[1]
    up = planes + RADIUS
    starts = []
    for stage in range(1, len(STAGES)):
        first = first_of(stage) - STAGES[0]
        starts.append((up + RADIUS - first - STAGES[stage], first))
    for k, (higher, lower) in enumerate(starts):
        for out, start in ((outs[2 * k], higher), (outs[2 * k + 1], lower)):
            count = out.shape[0]
            out[:, :EDGE, :] = before[start : start + count]
            out[:, EDGE : EDGE + rows, :] = conv[start : start + count]
            out[:, EDGE + rows :, :] = after[start : start + count]


def edges(conv, before, after):
    rows, columns = conv.shape[1:]
    shapes = []
    for stage in range(1, len(STAGES)):
        shapes += [
            jax.ShapeDtypeStruct((STAGES[stage], rows + 2 * EDGE, columns), jnp.float32)
        ] * 2
    return pl.pallas_call(
        edges_kernel,
        out_shape=shapes,
        in_specs=vmem(3),
        out_specs=vmem(len(shapes)),
        compiler_params=params(16),
        cost_estimate=cost(5_000_000),
        name="edges",
    )(conv, before, after)


def stage_kernel(stage, conv, before, after, lower, upper, *sends):
    rows = conv.shape[1]
    count = STAGES[stage]
    kernel = hat((rows, rows + 2 * EDGE), -EDGE).astype(jnp.float32).astype(jnp.bfloat16)
    side = 3 * EDGE
    out_row = lax.broadcasted_iota(jnp.int32, (2 * EDGE, 2 * side), 0)
    in_row = lax.broadcasted_iota(jnp.int32, (2 * EDGE, 2 * side), 1)
    out_last, in_last = out_row >= EDGE, in_row >= side
    distance = jnp.abs(
        (in_row - jnp.where(in_last, side + EDGE, 0))
        - (out_row - jnp.where(out_last, EDGE, 0))
        - jnp.where(in_last, 0, EDGE)
    )
    corner = jnp.where(out_last == in_last, jnp.maximum(BOX - distance, 0), 0)
    corner = corner.astype(jnp.float32).astype(jnp.bfloat16)
    me = lax.axis_index("gx")
    for d in range(4):
        quarter = lax.rem(me + d, 4)
        take_lower = (quarter == 0).astype(jnp.float32)
        take_upper = (quarter == 3).astype(jnp.float32)
        base = RADIUS + 8 * quarter + plane_offset(stage, quarter)
        for j in range(count):
            plane = jnp.concatenate([before[base + j], conv[base + j], after[base + j]], axis=0)
            plane = plane + take_lower * lower[j] + take_upper * upper[j]
            sends[d][j * rows : (j + 1) * rows, :] = along_rows(kernel, plane)
        if stage == 1:
            base = RADIUS + 8 * quarter + plane_offset(0, quarter)
            for j in range(STAGES[0]):
                part = jnp.concatenate(
                    [
                        before[base + j],
                        conv[base + j, : 2 * EDGE, :],
                        conv[base + j, rows - 2 * EDGE :, :],
                        after[base + j],
                    ],
                    axis=0,
                )
                at = count * rows + j * 2 * EDGE
                sends[d][at : at + 2 * EDGE, :] = along_rows(corner, part)


def stage_sends(stage, conv, before, after, lower, upper):
    rows, columns = conv.shape[1:]
    total = STAGES[stage] * rows + (STAGES[0] * 2 * EDGE if stage == 1 else 0)
    return pl.pallas_call(
        functools.partial(stage_kernel, stage),
        out_shape=[jax.ShapeDtypeStruct((total, columns), jnp.float32)] * 4,
        in_specs=vmem(5),
        out_specs=vmem(4),
        compiler_params=params(20),
        cost_estimate=cost(40_000_000),
    )(conv, before, after, lower, upper)


def finish_kernel(stage, *refs):
    aliased = 0 if stage == 0 else 2
    scale, plane_scale, own, up, across, down = refs[:6]
    filtered, projected = refs[6 + aliased : 8 + aliased]
    smooth, sharp, sem = refs[8 + aliased :]
    columns = own.shape[-1]
    half = columns // 2
    me = lax.axis_index("gx")
    center = hat((columns, columns), 0)
    row = lax.broadcasted_iota(jnp.int32, (columns, columns), 0)
    column = lax.broadcasted_iota(jnp.int32, (columns, columns), 1)
    place = jnp.where(row < half, row - half, row + half)
    outer = jnp.maximum(BOX - jnp.abs(place - column), 0)
    weights = jnp.concatenate([center, center, outer, outer], axis=0)
    weights = weights.astype(jnp.float32).astype(jnp.bfloat16)
    top = jnp.tanh(jnp.float32(sharpness * threshold))
    inverse = 1.0 / (top + jnp.tanh(jnp.float32(sharpness * (1.0 - threshold))))

    sources = [up, own, down, across]

    def rows_of(take, put_rows, scale_rows, plane_factor):
        values = [take(source) for source in sources]
        for r in range(4):
            block = lax.rem(me + 3 + r, 4)
            has_before = (block != 0).astype(jnp.float32)
            has_after = (block != 3).astype(jnp.float32)
            outer_values = jnp.concatenate(
                [
                    values[(r + 3) % 4][:, half:] * has_before,
                    values[(r + 1) % 4][:, :half] * has_after,
                ],
                axis=1,
            )
            parts = two_parts(values[r]) + two_parts(outer_values)
            summed = jnp.dot(
                jnp.concatenate(parts, axis=1), weights, preferred_element_type=jnp.float32
            )
            lanes = pl.ds(pl.multiple_of(block * columns, columns), columns)
            smoothed = summed * (scale[scale_rows, lanes] * plane_factor)
            smooth[put_rows, lanes] = smoothed
            sharp[put_rows, lanes] = (
                top + jnp.tanh(sharpness * (smoothed - threshold))
            ) * inverse

    copies = []

    def send(buffer_rows, plane, rows):
        for source, target in ((smooth, filtered), (sharp, projected)):
            copy = pltpu.make_async_copy(
                source.at[buffer_rows, :], target.at[plane, rows, :], sem.at[len(copies)]
            )
            copy.start()
            copies.append(copy)

    offset = plane_offset(stage, me)
    rows = scale.shape[0]
    if stage == 0:
        inner = rows - 2 * EDGE
        for j in range(STAGES[0]):
            here = slice(j * inner, (j + 1) * inner)
            rows_of(lambda s: s[j], here, slice(EDGE, rows - EDGE), plane_scale[offset + j])
            send(pl.ds(j * inner, inner), offset + j, pl.ds(EDGE, inner))
    else:
        for j in range(STAGES[stage]):
            here = slice(j * rows, (j + 1) * rows)
            rows_of(lambda s: s[here, :], here, slice(0, rows), plane_scale[offset + j])
            send(pl.ds(j * rows, rows), offset + j, pl.ds(0, rows))
    if stage == 1:
        first = plane_offset(0, me)
        at = STAGES[stage] * rows
        for j in range(STAGES[0]):
            for put in (0, rows - EDGE):
                here = slice(at, at + EDGE)
                rows_of(
                    lambda s: s[here, :], here, slice(put, put + EDGE), plane_scale[first + j]
                )
                send(pl.ds(at, EDGE), first + j, pl.ds(put, EDGE))
                at += EDGE
    for copy in copies:
        copy.wait()


def finish(stage, scale, plane_scale, received, results):
    rows, width = scale.shape
    whole = jax.ShapeDtypeStruct((plane_scale.shape[0], rows, width), jnp.float32)
    count = received[0].size // received[0].shape[-1]
    copies = 2 * STAGES[stage] + (4 * STAGES[0] if stage == 1 else 0)
    return pl.pallas_call(
        functools.partial(finish_kernel, stage),
        out_shape=[whole, whole],
        in_specs=[
            pl.BlockSpec(memory_space=pltpu.VMEM),
            pl.BlockSpec(memory_space=pltpu.SMEM),
        ]
        + vmem(4)
        + [pl.BlockSpec(memory_space=pl.ANY)] * len(results),
        out_specs=[pl.BlockSpec(memory_space=pl.ANY)] * 2,
        scratch_shapes=[
            pltpu.VMEM((count, width), jnp.float32),
            pltpu.VMEM((count, width), jnp.float32),
            pltpu.SemaphoreType.DMA((copies,)),
        ],
        input_output_aliases={6: 0, 7: 1} if results else {},
        compiler_params=params(20),
        cost_estimate=cost(40_000_000),
    )(scale, plane_scale, *received, *results)


def one_side(reach):
    return reach * (RADIUS + 1) - reach * (reach + 1) // 2


def edge_sums(start, length, length_all):
    position = start + lax.iota(jnp.int32, length)
    reach_left = jnp.minimum(position, RADIUS)
    reach_right = jnp.minimum(length_all - 1 - position, RADIUS)
    return (RADIUS + 1 + one_side(reach_left) + one_side(reach_right)).astype(jnp.float32)


def shifted(block, axis, distance):
    peers = lax.axis_size(axis)
    route = [(i, i + distance) for i in range(peers) if 0 <= i + distance < peers]
    return lax.ppermute(block, axis, route)


def turned(block, distance):
    peers = lax.axis_size("gx")
    return lax.ppermute(block, "gx", [(i, (i + distance) % peers) for i in range(peers)])


def around(sends):
    return [sends[0]] + [turned(sends[d], d) for d in (1, 2, 3)]


def program(density, mask):
    planes, row_count, columns = density.shape
    groups = lax.axis_size("gx")
    layers = planes // groups
    width = columns * groups
    count_x = edge_sums(0, width, width)
    count_y = edge_sums(
        lax.axis_index("gy") * row_count, row_count, row_count * lax.axis_size("gy")
    )
    count_z = edge_sums(
        lax.axis_index(("gz", "gx")) * layers, layers, planes * lax.axis_size("gz")
    )
    scale = 1.0 / (count_y[:, None] * count_x[None, :])
    plane_scale = 1.0 / count_z

    conv, first_rows, last_rows, *sends = section(density, mask)
    received = [around(sends)]
    before = shifted(last_rows, "gy", 1)
    after = shifted(first_rows, "gy", -1)
    outgoing = edges(conv, before, after)
    halos = []
    for k in range(len(STAGES) - 1):
        halos.append((shifted(outgoing[2 * k], "gz", 1), shifted(outgoing[2 * k + 1], "gz", -1)))
    for stage in range(1, len(STAGES)):
        sends = stage_sends(stage, conv, before, after, *halos[stage - 1])
        received.append(around(sends))
    results = []
    for stage in range(len(STAGES)):
        results = finish(stage, scale, plane_scale, received[stage], results)
    return tuple(results)


def solution(mesh):
    placed = (P("gz", "gy", "gx"), P("gz", "gy", "gx"))
    return jax.shard_map(
        program,
        mesh=mesh,
        in_specs=placed,
        out_specs=(P(("gz", "gx"), "gy", None), P(("gz", "gx"), "gy", None)),
        check_vma=False,
    )
```

```python
import functools

import jax
import jax.numpy as jnp
from jax import lax
from jax.experimental import pallas as pl
from jax.experimental.pallas import tpu as pltpu
from jax.sharding import PartitionSpec as P


RADIUS = 6
CELLS = 8
EDGE = 8
BOX = RADIUS + 1

sharpness = 8.0
threshold = 0.5


STAGES = (2, 2, 4)
CHUNKS = 4


def first_of(stage):
    return sum(STAGES[:stage])


def plane_offset(stage, quarter):
    ascending = first_of(stage)
    descending = sum(STAGES) - ascending - STAGES[stage]
    return jnp.where(quarter == 0, descending, ascending)


def hat(shape, shift):
    out_index = lax.broadcasted_iota(jnp.int32, shape, 0)
    in_index = lax.broadcasted_iota(jnp.int32, shape, 1)
    distance = jnp.abs(in_index + shift - out_index)
    return jnp.maximum(BOX - distance, 0)


def two_parts(values):
    high = values.astype(jnp.bfloat16)
    low = (values - high.astype(jnp.float32)).astype(jnp.bfloat16)
    return high, low


def along_rows(kernel, values):
    high, low = two_parts(values)
    return jnp.dot(kernel, high, preferred_element_type=jnp.float32) + jnp.dot(
        kernel, low, preferred_element_type=jnp.float32
    )


def vmem(count):
    return [pl.BlockSpec(memory_space=pltpu.VMEM)] * count


def params(mib):
    return pltpu.CompilerParams(vmem_limit_bytes=mib * 1024 * 1024)


def cost(flops):
    return pl.CostEstimate(flops=flops, bytes_accessed=8 * 1024 * 1024, transcendentals=0)


def section_kernel(density, mask, conv, *rest):
    near_edges, far_edges, sends = rest[:2], rest[2:4], rest[4:8]
    held, table, codes, sems = rest[8:]
    planes, rows, columns = density.shape
    blocks = rows // CELLS
    copy_mask = pltpu.make_async_copy(mask, table, sems.at[CHUNKS])
    copy_mask.start()
    copies = []
    for c in range(CHUNKS):
        part = pl.ds(c * (rows // CHUNKS), rows // CHUNKS)
        copies.append(
            pltpu.make_async_copy(density.at[:, part, :], held.at[:, part, :], sems.at[c])
        )
        copies[-1].start()
    spread = (
        lax.broadcasted_iota(jnp.int32, (columns // CELLS, columns), 1) // CELLS
        == lax.broadcasted_iota(jnp.int32, (columns // CELLS, columns), 0)
    )
    copy_mask.wait()
    codes[...] = jnp.dot(
        table[...]
        .reshape(planes // CELLS * blocks, columns // CELLS)
        .astype(jnp.float32)
        .astype(jnp.bfloat16),
        spread.astype(jnp.float32).astype(jnp.bfloat16),
        preferred_element_type=jnp.float32,
    )

    def tile(i, carry):
        row = pl.ds(pl.multiple_of(i * CELLS, CELLS), CELLS)
        values, boxes = [], []
        box = total = None
        for z in range(planes + 2 * RADIUS):
            if z < planes:
                if z % CELLS == 0:
                    code = jnp.broadcast_to(
                        codes[pl.ds(z // CELLS * blocks + i, 1), :], (CELLS, columns)
                    )
                    void, solid = code < 0.5, code < 1.5
                value = jnp.where(void, 0.0, jnp.where(solid, 1.0, held[z, row, :]))
                values.append(value)
                box = value if box is None else box + value
            if z < planes + RADIUS:
                if z >= BOX:
                    box = box - values[z - BOX]
                boxes.append(box)
                total = box if total is None else total + box
            if z >= BOX:
                total = total - boxes[z - BOX]
            conv[z, row, :] = total
        return carry

    for c in range(CHUNKS):
        copies[c].wait()
        lax.fori_loop(c * blocks // CHUNKS, (c + 1) * blocks // CHUNKS, tile, 0)
    for k, part in enumerate((slice(0, EDGE), slice(rows - EDGE, rows))):
        near_edges[k][:RADIUS] = conv[:RADIUS, part, :]
        near_edges[k][RADIUS:] = conv[planes + RADIUS :, part, :]
        far_edges[k][...] = conv[RADIUS : planes + RADIUS, part, :]
    kernel = hat((rows - 2 * EDGE, rows), -EDGE).astype(jnp.float32).astype(jnp.bfloat16)
    me = lax.axis_index("gx")
    for distance in range(4):
        quarter = lax.rem(me + distance, 4)
        base = RADIUS + 8 * quarter + plane_offset(0, quarter)
        for j in range(STAGES[0]):
            sends[distance][j] = along_rows(kernel, conv[base + j])


def section(density, mask):
    planes, rows, columns = density.shape
    span = planes + 2 * RADIUS
    f32 = functools.partial(jax.ShapeDtypeStruct, dtype=jnp.float32)
    return pl.pallas_call(
        section_kernel,
        out_shape=[f32((span, rows, columns))]
        + [f32((2 * RADIUS, EDGE, columns))] * 2
        + [f32((planes, EDGE, columns))] * 2
        + [f32((STAGES[0], rows - 2 * EDGE, columns))] * 4,
        in_specs=[pl.BlockSpec(memory_space=pltpu.HBM)] * 2,
        out_specs=vmem(9),
        scratch_shapes=[
            pltpu.VMEM(density.shape, jnp.float32),
            pltpu.VMEM(mask.shape, jnp.int32),
            pltpu.VMEM((planes // CELLS * rows // CELLS, columns), jnp.float32),
            pltpu.SemaphoreType.DMA((CHUNKS + 1,)),
        ],
        compiler_params=params(24),
        cost_estimate=cost(40_000_000),
        name="section",
    )(
        pltpu.with_memory_space_constraint(density, pltpu.HBM),
        pltpu.with_memory_space_constraint(mask, pltpu.HBM),
    )


def inside(axis, first):
    place = lax.axis_index(axis)
    edge = 0 if first else lax.axis_size(axis) - 1
    return (place != edge).astype(jnp.float32)


def edges_kernel(conv, before, after, *outs):
    planes = conv.shape[0] - 2 * RADIUS
    rows = conv.shape[1]
    has_before, has_after = inside("gy", True), inside("gy", False)
    for stage in range(1, len(STAGES)):
        first = first_of(stage) - STAGES[0]
        count = STAGES[stage]
        higher, lower = outs[2 * stage - 2 : 2 * stage]
        for out, start in ((higher, 2 * RADIUS - first - count), (lower, first)):
            at = start if start < RADIUS else start + planes
            out[:, :EDGE, :] = before[start : start + count] * has_before
            out[:, EDGE : EDGE + rows, :] = conv[at : at + count]
            out[:, EDGE + rows :, :] = after[start : start + count] * has_after


def edges(conv, before, after):
    rows, columns = conv.shape[1:]
    shapes = []
    for stage in range(1, len(STAGES)):
        shapes += [
            jax.ShapeDtypeStruct((STAGES[stage], rows + 2 * EDGE, columns), jnp.float32)
        ] * 2
    return pl.pallas_call(
        edges_kernel,
        out_shape=shapes,
        in_specs=vmem(3),
        out_specs=vmem(len(shapes)),
        compiler_params=params(8),
        cost_estimate=cost(5_000_000),
        name="edges",
    )(conv, before, after)


def stage_kernel(stage, conv, before, after, lower, upper, *sends):
    rows = conv.shape[1]
    count = STAGES[stage]
    kernel = hat((rows, rows + 2 * EDGE), -EDGE).astype(jnp.float32).astype(jnp.bfloat16)
    side = 3 * EDGE
    out_row = lax.broadcasted_iota(jnp.int32, (2 * EDGE, 2 * side), 0)
    in_row = lax.broadcasted_iota(jnp.int32, (2 * EDGE, 2 * side), 1)
    out_last, in_last = out_row >= EDGE, in_row >= side
    distance = jnp.abs(
        (in_row - jnp.where(in_last, side + EDGE, 0))
        - (out_row - jnp.where(out_last, EDGE, 0))
        - jnp.where(in_last, 0, EDGE)
    )
    corner = jnp.where(out_last == in_last, jnp.maximum(BOX - distance, 0), 0)
    corner = corner.astype(jnp.float32).astype(jnp.bfloat16)
    me = lax.axis_index("gx")
    has_before, has_after = inside("gy", True), inside("gy", False)
    for d in range(4):
        quarter = lax.rem(me + d, 4)
        take_lower = (quarter == 0).astype(jnp.float32) * inside("gz", True)
        take_upper = (quarter == 3).astype(jnp.float32) * inside("gz", False)
        base = 8 * quarter + plane_offset(stage, quarter)
        for j in range(count):
            plane = jnp.concatenate(
                [
                    before[base + j] * has_before,
                    conv[RADIUS + base + j],
                    after[base + j] * has_after,
                ],
                axis=0,
            )
            plane = plane + take_lower * lower[j] + take_upper * upper[j]
            sends[d][j * rows : (j + 1) * rows, :] = along_rows(kernel, plane)
        if stage == 1:
            base = 8 * quarter + plane_offset(0, quarter)
            for j in range(STAGES[0]):
                part = jnp.concatenate(
                    [
                        before[base + j] * has_before,
                        conv[RADIUS + base + j, : 2 * EDGE, :],
                        conv[RADIUS + base + j, rows - 2 * EDGE :, :],
                        after[base + j] * has_after,
                    ],
                    axis=0,
                )
                at = count * rows + j * 2 * EDGE
                sends[d][at : at + 2 * EDGE, :] = along_rows(corner, part)


def stage_sends(stage, conv, before, after, lower, upper):
    rows, columns = conv.shape[1:]
    total = STAGES[stage] * rows + (STAGES[0] * 2 * EDGE if stage == 1 else 0)
    return pl.pallas_call(
        functools.partial(stage_kernel, stage),
        out_shape=[jax.ShapeDtypeStruct((total, columns), jnp.float32)] * 4,
        in_specs=vmem(5),
        out_specs=vmem(4),
        compiler_params=params(20),
        cost_estimate=cost(40_000_000),
    )(conv, before, after, lower, upper)


def finish_kernel(stage, *refs):
    aliased = 0 if stage == 0 else 2
    scale, plane_scale, own, up, across, down = refs[:6]
    filtered, projected = refs[6 + aliased : 8 + aliased]
    smooth, sharp, sem = refs[8 + aliased :]
    columns = own.shape[-1]
    half = columns // 2
    me = lax.axis_index("gx")
    center = hat((columns, columns), 0)
    row = lax.broadcasted_iota(jnp.int32, (columns, columns), 0)
    column = lax.broadcasted_iota(jnp.int32, (columns, columns), 1)
    place = jnp.where(row < half, row - half, row + half)
    outer = jnp.maximum(BOX - jnp.abs(place - column), 0)
    weights = jnp.concatenate([center, center, outer, outer], axis=0)
    weights = weights.astype(jnp.float32).astype(jnp.bfloat16)
    top = jnp.tanh(jnp.float32(sharpness * threshold))
    inverse = 1.0 / (top + jnp.tanh(jnp.float32(sharpness * (1.0 - threshold))))

    sources = [up, own, down, across]

    def rows_of(take, put_rows, scale_rows, plane_factor):
        values = [take(source) for source in sources]
        for r in range(4):
            block = lax.rem(me + 3 + r, 4)
            has_before = (block != 0).astype(jnp.float32)
            has_after = (block != 3).astype(jnp.float32)
            outer_values = jnp.concatenate(
                [
                    values[(r + 3) % 4][:, half:] * has_before,
                    values[(r + 1) % 4][:, :half] * has_after,
                ],
                axis=1,
            )
            parts = two_parts(values[r]) + two_parts(outer_values)
            summed = jnp.dot(
                jnp.concatenate(parts, axis=1), weights, preferred_element_type=jnp.float32
            )
            lanes = pl.ds(pl.multiple_of(block * columns, columns), columns)
            smoothed = summed * (scale[scale_rows, lanes] * plane_factor)
            smooth[put_rows, lanes] = smoothed
            sharp[put_rows, lanes] = (
                top + jnp.tanh(sharpness * (smoothed - threshold))
            ) * inverse

    copies = []

    def send(buffer_rows, plane, rows):
        for source, target in ((smooth, filtered), (sharp, projected)):
            copy = pltpu.make_async_copy(
                source.at[buffer_rows, :], target.at[plane, rows, :], sem.at[len(copies)]
            )
            copy.start()
            copies.append(copy)

    offset = plane_offset(stage, me)
    rows = scale.shape[0]
    if stage == 0:
        inner = rows - 2 * EDGE
        for j in range(STAGES[0]):
            here = slice(j * inner, (j + 1) * inner)
            rows_of(lambda s: s[j], here, slice(EDGE, rows - EDGE), plane_scale[pl.ds(offset + j, 1), :])
            send(pl.ds(j * inner, inner), offset + j, pl.ds(EDGE, inner))
    else:
        for j in range(STAGES[stage]):
            here = slice(j * rows, (j + 1) * rows)
            rows_of(lambda s: s[here, :], here, slice(0, rows), plane_scale[pl.ds(offset + j, 1), :])
            send(pl.ds(j * rows, rows), offset + j, pl.ds(0, rows))
    if stage == 1:
        first = plane_offset(0, me)
        at = STAGES[stage] * rows
        for j in range(STAGES[0]):
            for put in (0, rows - EDGE):
                here = slice(at, at + EDGE)
                rows_of(
                    lambda s: s[here, :], here, slice(put, put + EDGE), plane_scale[pl.ds(first + j, 1), :]
                )
                send(pl.ds(at, EDGE), first + j, pl.ds(put, EDGE))
                at += EDGE
    for copy in copies:
        copy.wait()


def finish(stage, scale, plane_scale, received, results):
    rows, width = scale.shape
    whole = jax.ShapeDtypeStruct((plane_scale.shape[0], rows, width), jnp.float32)
    count = received[0].size // received[0].shape[-1]
    copies = 2 * STAGES[stage] + (4 * STAGES[0] if stage == 1 else 0)
    return pl.pallas_call(
        functools.partial(finish_kernel, stage),
        out_shape=[whole, whole],
        in_specs=vmem(6)
        + [pl.BlockSpec(memory_space=pl.ANY)] * len(results),
        out_specs=[pl.BlockSpec(memory_space=pl.ANY)] * 2,
        scratch_shapes=[
            pltpu.VMEM((count, width), jnp.float32),
            pltpu.VMEM((count, width), jnp.float32),
            pltpu.SemaphoreType.DMA((copies,)),
        ],
        input_output_aliases={6: 0, 7: 1} if results else {},
        compiler_params=params(20),
        cost_estimate=cost(40_000_000),
    )(scale, plane_scale, *received, *results)


def one_side(reach):
    return reach * (RADIUS + 1) - reach * (reach + 1) // 2


def edge_sums(position, length):
    reach_left = jnp.minimum(position, RADIUS)
    reach_right = jnp.minimum(length - 1 - position, RADIUS)
    return (RADIUS + 1 + one_side(reach_left) + one_side(reach_right)).astype(jnp.float32)


def scale_kernel(scale, plane_scale):
    rows, width = scale.shape
    layers = plane_scale.shape[0]
    row = lax.axis_index("gy") * rows + lax.broadcasted_iota(jnp.int32, (rows, 128), 0)
    count_y = edge_sums(row, rows * lax.axis_size("gy"))
    for c in range(width // 128):
        column = c * 128 + lax.broadcasted_iota(jnp.int32, (8, 128), 1)
        count_x = edge_sums(column, width)[:1]
        scale[:, c * 128 : (c + 1) * 128] = 1.0 / (count_y * count_x)
    section_place = lax.axis_index("gz") * lax.axis_size("gx") + lax.axis_index("gx")
    plane = section_place * layers + lax.broadcasted_iota(jnp.int32, plane_scale.shape, 0)
    plane_scale[...] = 1.0 / edge_sums(
        plane, layers * lax.axis_size("gx") * lax.axis_size("gz")
    )


def scales(rows, width, columns, layers):
    return pl.pallas_call(
        scale_kernel,
        out_shape=[
            jax.ShapeDtypeStruct((rows, width), jnp.float32),
            jax.ShapeDtypeStruct((layers, columns), jnp.float32),
        ],
        out_specs=vmem(2),
        compiler_params=params(4),
        cost_estimate=cost(5_000_000),
        name="scales",
    )()


def shifted(block, axis, distance):
    peers = lax.axis_size(axis)
    route = [(i, (i + distance) % peers) for i in range(peers)]
    return lax.ppermute(block, axis, route)


def around(sends):
    return [sends[0]] + [shifted(sends[d], "gx", d) for d in (1, 2, 3)]


def program(density, mask):
    planes, row_count, columns = density.shape
    groups = lax.axis_size("gx")
    layers = planes // groups
    width = columns * groups
    conv, near_first, near_last, far_first, far_last, *sends = section(density, mask)
    received = [around(sends)]
    near_before = shifted(near_last, "gy", 1)
    near_after = shifted(near_first, "gy", -1)
    before = shifted(far_last, "gy", 1)
    after = shifted(far_first, "gy", -1)
    outgoing = edges(conv, near_before, near_after)
    scale, plane_scale = scales(row_count, width, columns, layers)
    halos = []
    for k in range(len(STAGES) - 1):
        halos.append((shifted(outgoing[2 * k], "gz", 1), shifted(outgoing[2 * k + 1], "gz", -1)))
    for stage in range(1, len(STAGES)):
        sends = stage_sends(stage, conv, before, after, *halos[stage - 1])
        received.append(around(sends))
    results = []
    for stage in range(len(STAGES)):
        results = finish(stage, scale, plane_scale, received[stage], results)
    return tuple(results)


def solution(mesh):
    placed = (P("gz", "gy", "gx"), P("gz", "gy", "gx"))
    return jax.shard_map(
        program,
        mesh=mesh,
        in_specs=placed,
        out_specs=(P(("gz", "gx"), "gy", None), P(("gz", "gx"), "gy", None)),
        check_vma=False,
    )
```

```python
import functools

import jax
import jax.numpy as jnp
from jax import lax
from jax.experimental import pallas as pl
from jax.experimental.pallas import tpu as pltpu
from jax.sharding import PartitionSpec as P


RADIUS = 6
CELLS = 8
EDGE = 8
BOX = RADIUS + 1

sharpness = 8.0
threshold = 0.5


STAGES = (2, 1, 2, 3)
CHUNKS = 4


def first_of(stage):
    return sum(STAGES[:stage])


def both_offsets(stage):
    ascending = first_of(stage)
    return sum(STAGES) - ascending - STAGES[stage], ascending


def plane_offset(stage, quarter):
    descending, ascending = both_offsets(stage)
    return jnp.where(quarter == 0, descending, ascending)


def planes_of(stage):
    places = []
    for quarter in range(4):
        start = RADIUS + sum(STAGES) * quarter + both_offsets(stage)[min(quarter, 1)]
        places += range(start, start + STAGES[stage])
    return places


def outer_planes():
    span = 4 * sum(STAGES) + 2 * RADIUS
    return list(range(RADIUS)) + list(range(span - RADIUS, span))


NEAR = outer_planes() + planes_of(0) + planes_of(1)
FAR = [place for stage in range(2, len(STAGES)) for place in planes_of(stage)]


def hat(shape, shift):
    out_index = lax.broadcasted_iota(jnp.int32, shape, 0)
    in_index = lax.broadcasted_iota(jnp.int32, shape, 1)
    distance = jnp.abs(in_index + shift - out_index)
    return jnp.maximum(BOX - distance, 0)


def two_parts(values):
    high = values.astype(jnp.bfloat16)
    low = (values - high.astype(jnp.float32)).astype(jnp.bfloat16)
    return high, low


def along_rows(kernel, values):
    high, low = two_parts(values)
    return jnp.dot(kernel, high, preferred_element_type=jnp.float32) + jnp.dot(
        kernel, low, preferred_element_type=jnp.float32
    )


def vmem(count):
    return [pl.BlockSpec(memory_space=pltpu.VMEM)] * count


def params(mib):
    return pltpu.CompilerParams(vmem_limit_bytes=mib * 1024 * 1024)


def cost(flops):
    return pl.CostEstimate(flops=flops, bytes_accessed=8 * 1024 * 1024, transcendentals=0)


def section_kernel(density, mask, conv, *rest):
    near_edges, far_edges, sends = rest[:2], rest[2:4], rest[4:8]
    held, table, codes, sems = rest[8:]
    planes, rows, columns = density.shape
    blocks = rows // CELLS
    copy_mask = pltpu.make_async_copy(mask, table, sems.at[CHUNKS])
    copy_mask.start()
    copies = []
    for c in range(CHUNKS):
        part = pl.ds(c * (rows // CHUNKS), rows // CHUNKS)
        copies.append(
            pltpu.make_async_copy(density.at[:, part, :], held.at[:, part, :], sems.at[c])
        )
        copies[-1].start()
    spread = (
        lax.broadcasted_iota(jnp.int32, (columns // CELLS, columns), 1) // CELLS
        == lax.broadcasted_iota(jnp.int32, (columns // CELLS, columns), 0)
    )
    copy_mask.wait()
    codes[...] = jnp.dot(
        table[...]
        .reshape(planes // CELLS * blocks, columns // CELLS)
        .astype(jnp.float32)
        .astype(jnp.bfloat16),
        spread.astype(jnp.float32).astype(jnp.bfloat16),
        preferred_element_type=jnp.float32,
    )

    def tile(i, carry):
        row = pl.ds(pl.multiple_of(i * CELLS, CELLS), CELLS)
        values, boxes = [], []
        box = total = None
        for z in range(planes + 2 * RADIUS):
            if z < planes:
                if z % CELLS == 0:
                    code = jnp.broadcast_to(
                        codes[pl.ds(z // CELLS * blocks + i, 1), :], (CELLS, columns)
                    )
                    fixed, given = code < 1.5, jnp.where(code < 0.5, 0.0, 1.0)
                value = jnp.where(fixed, given, held[z, row, :])
                values.append(value)
                change = value - values[z - BOX] if z >= BOX else value
                box = change if box is None else box + change
            elif z < planes + RADIUS:
                box = box - values[z - BOX]
            if z < planes + RADIUS:
                boxes.append(box)
                change = box - boxes[z - BOX] if z >= BOX else box
                total = change if total is None else total + change
            else:
                total = total - boxes[z - BOX]
            conv[z, row, :] = total
        return carry

    for c in range(CHUNKS):
        copies[c].wait()
        lax.fori_loop(c * blocks // CHUNKS, (c + 1) * blocks // CHUNKS, tile, 0)
    for k, part in enumerate((slice(0, EDGE), slice(rows - EDGE, rows))):
        for edge, places in ((near_edges[k], NEAR), (far_edges[k], FAR)):
            for at, place in enumerate(places):
                edge[at] = conv[place, part, :]
    kernel = hat((rows - 2 * EDGE, rows), -EDGE).astype(jnp.float32).astype(jnp.bfloat16)
    me = lax.axis_index("gx")
    for distance in range(4):
        quarter = lax.rem(me + distance, 4)
        base = RADIUS + 8 * quarter + plane_offset(0, quarter)
        for j in range(STAGES[0]):
            sends[distance][j] = along_rows(kernel, conv[base + j])


def section(density, mask):
    planes, rows, columns = density.shape
    span = planes + 2 * RADIUS
    f32 = functools.partial(jax.ShapeDtypeStruct, dtype=jnp.float32)
    return pl.pallas_call(
        section_kernel,
        out_shape=[f32((span, rows, columns))]
        + [f32((len(NEAR), EDGE, columns))] * 2
        + [f32((len(FAR), EDGE, columns))] * 2
        + [f32((STAGES[0], rows - 2 * EDGE, columns))] * 4,
        in_specs=[pl.BlockSpec(memory_space=pltpu.HBM)] * 2,
        out_specs=vmem(9),
        scratch_shapes=[
            pltpu.VMEM(density.shape, jnp.float32),
            pltpu.VMEM(mask.shape, jnp.int32),
            pltpu.VMEM((planes // CELLS * rows // CELLS, columns), jnp.float32),
            pltpu.SemaphoreType.DMA((CHUNKS + 1,)),
        ],
        compiler_params=params(24),
        cost_estimate=cost(40_000_000),
        name="section",
    )(
        pltpu.with_memory_space_constraint(density, pltpu.HBM),
        pltpu.with_memory_space_constraint(mask, pltpu.HBM),
    )


def inside(axis, first):
    place = lax.axis_index(axis)
    edge = 0 if first else lax.axis_size(axis) - 1
    return (place != edge).astype(jnp.float32)


def edges_kernel(stages, conv, before, after, *outs):
    planes = conv.shape[0] - 2 * RADIUS
    rows = conv.shape[1]
    has_before, has_after = inside("gy", True), inside("gy", False)
    for k, stage in enumerate(stages):
        first = first_of(stage) - STAGES[0]
        count = STAGES[stage]
        higher, lower = outs[2 * k : 2 * k + 2]
        for out, start in ((higher, 2 * RADIUS - first - count), (lower, first)):
            at = start if start < RADIUS else start + planes
            out[:, :EDGE, :] = before[start : start + count] * has_before
            out[:, EDGE : EDGE + rows, :] = conv[at : at + count]
            out[:, EDGE + rows :, :] = after[start : start + count] * has_after


def edges(stages, conv, before, after):
    rows, columns = conv.shape[1:]
    shapes = []
    for stage in stages:
        shapes += [
            jax.ShapeDtypeStruct((STAGES[stage], rows + 2 * EDGE, columns), jnp.float32)
        ] * 2
    return pl.pallas_call(
        functools.partial(edges_kernel, stages),
        out_shape=shapes,
        in_specs=vmem(3),
        out_specs=vmem(len(shapes)),
        compiler_params=params(8),
        cost_estimate=cost(5_000_000),
        name="edges",
    )(conv, before, after)


def stage_kernel(stage, conv, before, after, lower, upper, *sends):
    rows = conv.shape[1]
    count = STAGES[stage]
    kernel = hat((rows, rows + 2 * EDGE), -EDGE).astype(jnp.float32).astype(jnp.bfloat16)
    side = 3 * EDGE
    out_row = lax.broadcasted_iota(jnp.int32, (2 * EDGE, 2 * side), 0)
    in_row = lax.broadcasted_iota(jnp.int32, (2 * EDGE, 2 * side), 1)
    out_last, in_last = out_row >= EDGE, in_row >= side
    distance = jnp.abs(
        (in_row - jnp.where(in_last, side + EDGE, 0))
        - (out_row - jnp.where(out_last, EDGE, 0))
        - jnp.where(in_last, 0, EDGE)
    )
    corner = jnp.where(out_last == in_last, jnp.maximum(BOX - distance, 0), 0)
    corner = corner.astype(jnp.float32).astype(jnp.bfloat16)
    me = lax.axis_index("gx")
    has_before, has_after = inside("gy", True), inside("gy", False)
    for d in range(4):
        quarter = lax.rem(me + d, 4)
        take_lower = (quarter == 0).astype(jnp.float32) * inside("gz", True)
        take_upper = (quarter == 3).astype(jnp.float32) * inside("gz", False)
        base = RADIUS + 8 * quarter + plane_offset(stage, quarter)
        if stage == 1:
            edge = len(NEAR) + count * (quarter - 4)
        else:
            edge = 4 * (first_of(stage) - first_of(2)) + count * quarter
        for j in range(count):
            plane = jnp.concatenate(
                [
                    before[edge + j] * has_before,
                    conv[base + j],
                    after[edge + j] * has_after,
                ],
                axis=0,
            )
            plane = plane + take_lower * lower[j] + take_upper * upper[j]
            sends[d][j * rows : (j + 1) * rows, :] = along_rows(kernel, plane)
        if stage == 1:
            base = RADIUS + 8 * quarter + plane_offset(0, quarter)
            edge = 2 * RADIUS + STAGES[0] * quarter
            for j in range(STAGES[0]):
                part = jnp.concatenate(
                    [
                        before[edge + j] * has_before,
                        conv[base + j, : 2 * EDGE, :],
                        conv[base + j, rows - 2 * EDGE :, :],
                        after[edge + j] * has_after,
                    ],
                    axis=0,
                )
                at = count * rows + j * 2 * EDGE
                sends[d][at : at + 2 * EDGE, :] = along_rows(corner, part)


def stage_sends(stage, conv, before, after, lower, upper):
    rows, columns = conv.shape[1:]
    total = STAGES[stage] * rows + (STAGES[0] * 2 * EDGE if stage == 1 else 0)
    return pl.pallas_call(
        functools.partial(stage_kernel, stage),
        out_shape=[jax.ShapeDtypeStruct((total, columns), jnp.float32)] * 4,
        in_specs=vmem(5),
        out_specs=vmem(4),
        compiler_params=params(20),
        cost_estimate=cost(40_000_000),
    )(conv, before, after, lower, upper)


def finish_kernel(stage, *refs):
    aliased = 0 if stage == 0 else 2
    scale, plane_scale, weights, own, up, across, down = refs[:7]
    filtered, projected = refs[7 + aliased : 9 + aliased]
    smooth, sharp, sem = refs[9 + aliased :]
    columns = own.shape[-1]
    half = columns // 2
    me = lax.axis_index("gx")
    top = jnp.tanh(jnp.float32(sharpness * threshold))
    inverse = 1.0 / (top + jnp.tanh(jnp.float32(sharpness * (1.0 - threshold))))

    sources = [up, own, down, across]

    def rows_of(take, put_rows, scale_rows, plane_factor):
        values = [take(source) for source in sources]
        for r in range(4):
            block = lax.rem(me + 3 + r, 4)
            has_before = (block != 0).astype(jnp.float32)
            has_after = (block != 3).astype(jnp.float32)
            outer_values = jnp.where(
                lax.broadcasted_iota(jnp.int32, (values[r].shape[0], half), 1) < half // 2,
                values[(r + 1) % 4][:, :half] * has_after,
                values[(r + 3) % 4][:, half:] * has_before,
            )
            parts = two_parts(values[r]) + two_parts(outer_values)
            summed = jnp.dot(
                jnp.concatenate(parts, axis=1), weights[...], preferred_element_type=jnp.float32
            )
            lanes = pl.ds(pl.multiple_of(block * columns, columns), columns)
            smoothed = summed * (scale[scale_rows, lanes] * plane_factor)
            smooth[put_rows, lanes] = smoothed
            sharp[put_rows, lanes] = (
                top + jnp.tanh(sharpness * (smoothed - threshold))
            ) * inverse

    copies = []

    def send(buffer_rows, plane, rows):
        for source, target in ((smooth, filtered), (sharp, projected)):
            copy = pltpu.make_async_copy(
                source.at[buffer_rows, :], target.at[plane, rows, :], sem.at[len(copies)]
            )
            copy.start()
            copies.append(copy)

    offset = plane_offset(stage, me)
    rows = scale.shape[0]
    if stage == 0:
        inner = rows - 2 * EDGE
        for j in range(STAGES[0]):
            here = slice(j * inner, (j + 1) * inner)
            rows_of(lambda s: s[j], here, slice(EDGE, rows - EDGE), plane_scale[pl.ds(offset + j, 1), :])
            send(pl.ds(j * inner, inner), offset + j, pl.ds(EDGE, inner))
    else:
        for j in range(STAGES[stage]):
            here = slice(j * rows, (j + 1) * rows)
            rows_of(lambda s: s[here, :], here, slice(0, rows), plane_scale[pl.ds(offset + j, 1), :])
            send(pl.ds(j * rows, rows), offset + j, pl.ds(0, rows))
    if stage == 1:
        first = plane_offset(0, me)
        at = STAGES[stage] * rows
        for j in range(STAGES[0]):
            for put in (0, rows - EDGE):
                here = slice(at, at + EDGE)
                rows_of(
                    lambda s: s[here, :], here, slice(put, put + EDGE), plane_scale[pl.ds(first + j, 1), :]
                )
                send(pl.ds(at, EDGE), first + j, pl.ds(put, EDGE))
                at += EDGE
    for copy in copies:
        copy.wait()


def finish(stage, scale, plane_scale, weights, received, results):
    rows, width = scale.shape
    whole = jax.ShapeDtypeStruct((plane_scale.shape[0], rows, width), jnp.float32)
    count = received[0].size // received[0].shape[-1]
    copies = 2 * STAGES[stage] + (4 * STAGES[0] if stage == 1 else 0)
    return pl.pallas_call(
        functools.partial(finish_kernel, stage),
        out_shape=[whole, whole],
        in_specs=vmem(7)
        + [pl.BlockSpec(memory_space=pl.ANY)] * len(results),
        out_specs=[pl.BlockSpec(memory_space=pl.ANY)] * 2,
        scratch_shapes=[
            pltpu.VMEM((count, width), jnp.float32),
            pltpu.VMEM((count, width), jnp.float32),
            pltpu.SemaphoreType.DMA((copies,)),
        ],
        input_output_aliases={7: 0, 8: 1} if results else {},
        compiler_params=params(20),
        cost_estimate=cost(40_000_000),
    )(scale, plane_scale, weights, *received, *results)


def one_side(reach):
    return reach * (RADIUS + 1) - reach * (reach + 1) // 2


def edge_sums(position, length):
    reach_left = jnp.minimum(position, RADIUS)
    reach_right = jnp.minimum(length - 1 - position, RADIUS)
    return (RADIUS + 1 + one_side(reach_left) + one_side(reach_right)).astype(jnp.float32)


def scale_kernel(scale, plane_scale, weights):
    rows, width = scale.shape
    layers = plane_scale.shape[0]
    row = lax.axis_index("gy") * rows + lax.broadcasted_iota(jnp.int32, (rows, 128), 0)
    count_y = edge_sums(row, rows * lax.axis_size("gy"))
    for c in range(width // 128):
        column = c * 128 + lax.broadcasted_iota(jnp.int32, (8, 128), 1)
        count_x = edge_sums(column, width)[:1]
        scale[:, c * 128 : (c + 1) * 128] = 1.0 / (count_y * count_x)
    section_place = lax.axis_index("gz") * lax.axis_size("gx") + lax.axis_index("gx")
    plane = section_place * layers + lax.broadcasted_iota(jnp.int32, plane_scale.shape, 0)
    plane_scale[...] = 1.0 / edge_sums(
        plane, layers * lax.axis_size("gx") * lax.axis_size("gz")
    )
    columns = weights.shape[1]
    half = columns // 2
    center = hat((columns, columns), 0)
    row = lax.broadcasted_iota(jnp.int32, (half, columns), 0)
    column = lax.broadcasted_iota(jnp.int32, (half, columns), 1)
    place = jnp.where(row < half // 2, row + columns, row - half)
    outer = jnp.maximum(BOX - jnp.abs(place - column), 0)
    at = 0
    for part in (center, center, outer, outer):
        weights[at : at + part.shape[0], :] = part.astype(jnp.float32).astype(jnp.bfloat16)
        at += part.shape[0]


def scales(rows, width, columns, layers):
    return pl.pallas_call(
        scale_kernel,
        out_shape=[
            jax.ShapeDtypeStruct((rows, width), jnp.float32),
            jax.ShapeDtypeStruct((layers, columns), jnp.float32),
            jax.ShapeDtypeStruct((3 * columns, columns), jnp.bfloat16),
        ],
        out_specs=vmem(3),
        compiler_params=params(4),
        cost_estimate=cost(5_000_000),
        name="scales",
    )()


def shifted(block, axis, distance):
    peers = lax.axis_size(axis)
    route = [(i, (i + distance) % peers) for i in range(peers)]
    return lax.ppermute(block, axis, route)


def around(sends):
    return [sends[0]] + [shifted(sends[d], "gx", d) for d in (1, 2, 3)]


def program(density, mask):
    planes, row_count, columns = density.shape
    groups = lax.axis_size("gx")
    layers = planes // groups
    width = columns * groups
    conv, near_first, near_last, far_first, far_last, *sends = section(density, mask)
    received = [around(sends)]
    near = (shifted(near_last, "gy", 1), shifted(near_first, "gy", -1))
    far = (shifted(far_last, "gy", 1), shifted(far_first, "gy", -1))
    outgoing = edges((1,), conv, *near)
    outgoing += edges(tuple(range(2, len(STAGES))), conv, *near)
    halos = []
    for k in range(len(STAGES) - 1):
        halos.append((shifted(outgoing[2 * k], "gz", 1), shifted(outgoing[2 * k + 1], "gz", -1)))
    tables = scales(row_count, width, columns, layers)
    for stage in range(1, len(STAGES)):
        ends = near if stage == 1 else far
        sends = stage_sends(stage, conv, *ends, *halos[stage - 1])
        received.append(around(sends))
    results = []
    for stage in range(len(STAGES)):
        results = finish(stage, *tables, received[stage], results)
    return tuple(results)


def solution(mesh):
    placed = (P("gz", "gy", "gx"), P("gz", "gy", "gx"))
    return jax.shard_map(
        program,
        mesh=mesh,
        in_specs=placed,
        out_specs=(P(("gz", "gx"), "gy", None), P(("gz", "gx"), "gy", None)),
        check_vma=False,
    )
```

```python
import functools

import jax
import jax.numpy as jnp
from jax import lax
from jax.experimental import pallas as pl
from jax.experimental.pallas import tpu as pltpu
from jax.sharding import PartitionSpec as P


RADIUS = 6
CELLS = 8
EDGE = 8
BOX = RADIUS + 1

sharpness = 8.0
threshold = 0.5


STAGES = (2, 2, 2, 2)
GROUPS = ((0, 1), (2,))
CHUNKS = 4


def first_of(stage):
    return sum(STAGES[:stage])


def both_offsets(stage):
    ascending = first_of(stage)
    return sum(STAGES) - ascending - STAGES[stage], ascending


def plane_offset(stage, quarter):
    descending, ascending = both_offsets(stage)
    return jnp.where(quarter == 0, descending, ascending)


def outer_places():
    span = 4 * sum(STAGES) + 2 * RADIUS
    places = {}
    for stage in range(1, len(STAGES)):
        first = first_of(stage) - STAGES[0]
        for j in range(STAGES[stage]):
            places[span - first - STAGES[stage] + j] = (stage, 0, j)
            places[first + j] = (stage, 1, j)
    return places


def hat(shape, shift):
    out_index = lax.broadcasted_iota(jnp.int32, shape, 0)
    in_index = lax.broadcasted_iota(jnp.int32, shape, 1)
    distance = jnp.abs(in_index + shift - out_index)
    return jnp.maximum(BOX - distance, 0)


def two_parts(values):
    high = values.astype(jnp.bfloat16)
    low = (values - high.astype(jnp.float32)).astype(jnp.bfloat16)
    return high, low


def along_rows(kernel, values):
    high, low = two_parts(values)
    return jnp.dot(kernel, high, preferred_element_type=jnp.float32) + jnp.dot(
        kernel, low, preferred_element_type=jnp.float32
    )


def vmem(count):
    return [pl.BlockSpec(memory_space=pltpu.VMEM)] * count


def params(mib):
    return pltpu.CompilerParams(vmem_limit_bytes=mib * 1024 * 1024)


def cost(flops):
    return pl.CostEstimate(flops=flops, bytes_accessed=8 * 1024 * 1024, transcendentals=0)


def section_kernel(density, mask, conv, *rest):
    sends, outer = rest[:4], rest[4:-4]
    held, table, codes, sems = rest[-4:]
    places = outer_places()
    planes, rows, columns = density.shape
    blocks = rows // CELLS
    copy_mask = pltpu.make_async_copy(mask, table, sems.at[CHUNKS])
    copy_mask.start()
    copies = []
    for c in range(CHUNKS):
        part = pl.ds(c * (rows // CHUNKS), rows // CHUNKS)
        copies.append(
            pltpu.make_async_copy(density.at[:, part, :], held.at[:, part, :], sems.at[c])
        )
        copies[-1].start()
    spread = (
        lax.broadcasted_iota(jnp.int32, (columns // CELLS, columns), 1) // CELLS
        == lax.broadcasted_iota(jnp.int32, (columns // CELLS, columns), 0)
    )
    copy_mask.wait()
    codes[...] = jnp.dot(
        table[...]
        .reshape(planes // CELLS * blocks, columns // CELLS)
        .astype(jnp.float32)
        .astype(jnp.bfloat16),
        spread.astype(jnp.float32).astype(jnp.bfloat16),
        preferred_element_type=jnp.float32,
    )

    def tile(i, carry):
        row = pl.ds(pl.multiple_of(i * CELLS, CELLS), CELLS)
        values, boxes = [], []
        box = total = None
        for z in range(planes + 2 * RADIUS):
            if z < planes:
                if z % CELLS == 0:
                    code = jnp.broadcast_to(
                        codes[pl.ds(z // CELLS * blocks + i, 1), :], (CELLS, columns)
                    )
                    fixed, given = code < 1.5, jnp.where(code < 0.5, 0.0, 1.0)
                value = jnp.where(fixed, given, held[z, row, :])
                values.append(value)
                change = value - values[z - BOX] if z >= BOX else value
                box = change if box is None else box + change
            elif z < planes + RADIUS:
                box = box - values[z - BOX]
            if z < planes + RADIUS:
                boxes.append(box)
                change = box - boxes[z - BOX] if z >= BOX else box
                total = change if total is None else total + change
            else:
                total = total - boxes[z - BOX]
            if z in places:
                stage, side, j = places[z]
                outer[2 * (stage - 1) + side][j, row, :] = total
            else:
                conv[z - RADIUS, row, :] = total
        return carry

    for c in range(CHUNKS):
        copies[c].wait()
        lax.fori_loop(c * blocks // CHUNKS, (c + 1) * blocks // CHUNKS, tile, 0)
    me = lax.axis_index("gx")
    for distance in range(4):
        quarter = lax.rem(me + distance, 4)
        base = 8 * quarter + plane_offset(0, quarter)
        for j in range(STAGES[0]):
            sends[distance][j] = conv[base + j]


def section(density, mask):
    planes, rows, columns = density.shape
    f32 = functools.partial(jax.ShapeDtypeStruct, dtype=jnp.float32)
    shapes = [f32(density.shape)] + [f32((STAGES[0], rows, columns))] * 4
    for count in STAGES[1:]:
        shapes += [f32((count, rows, columns))] * 2
    return pl.pallas_call(
        section_kernel,
        out_shape=shapes,
        in_specs=[pl.BlockSpec(memory_space=pltpu.HBM)] * 2,
        out_specs=vmem(len(shapes)),
        scratch_shapes=[
            pltpu.VMEM(density.shape, jnp.float32),
            pltpu.VMEM(mask.shape, jnp.int32),
            pltpu.VMEM((planes // CELLS * rows // CELLS, columns), jnp.float32),
            pltpu.SemaphoreType.DMA((CHUNKS + 1,)),
        ],
        compiler_params=params(24),
        cost_estimate=cost(40_000_000),
        name="section",
    )(
        pltpu.with_memory_space_constraint(density, pltpu.HBM),
        pltpu.with_memory_space_constraint(mask, pltpu.HBM),
    )


def inside(axis, first):
    place = lax.axis_index(axis)
    edge = 0 if first else lax.axis_size(axis) - 1
    return (place != edge).astype(jnp.float32)


def call(kernel, shapes, args, mib, flops=20_000_000):
    f32 = [jax.ShapeDtypeStruct(shape, jnp.float32) for shape in shapes]
    return pl.pallas_call(
        kernel,
        out_shape=f32,
        in_specs=vmem(len(args)),
        out_specs=vmem(len(f32)),
        compiler_params=params(mib),
        cost_estimate=cost(flops),
    )(*args)


def stage_kernel(stage, conv, lower, upper, *sends):
    me = lax.axis_index("gx")
    for d in range(4):
        quarter = lax.rem(me + d, 4)
        take_lower = (quarter == 0).astype(jnp.float32) * inside("gz", True)
        take_upper = (quarter == 3).astype(jnp.float32) * inside("gz", False)
        base = 8 * quarter + plane_offset(stage, quarter)
        for j in range(STAGES[stage]):
            sends[d][j] = conv[base + j] + take_lower * lower[j] + take_upper * upper[j]


def stage_sends(stage, conv, lower, upper):
    shapes = [(STAGES[stage],) + conv.shape[1:]] * 4
    kernel = functools.partial(stage_kernel, stage)
    return call(kernel, shapes, (conv, lower, upper), 12)


def fill_kernel(stage, conv, lower, upper, whole, first, last):
    count, rows = STAGES[stage], conv.shape[1]
    for quarter in range(4):
        base = 8 * quarter + both_offsets(stage)[min(quarter, 1)]
        for j in range(count):
            plane = conv[base + j]
            if quarter == 0:
                plane = plane + inside("gz", True) * lower[j]
            if quarter == 3:
                plane = plane + inside("gz", False) * upper[j]
            at = count * quarter + j
            whole[at] = plane
            first[at] = plane[:EDGE]
            last[at] = plane[rows - EDGE :]


def fill(stage, conv, lower, upper):
    total = 4 * STAGES[stage]
    shapes = [(total,) + conv.shape[1:]] + [(total, EDGE, conv.shape[2])] * 2
    kernel = functools.partial(fill_kernel, stage)
    return call(kernel, shapes, (conv, lower, upper), 12)


def row_weights(rows):
    return hat((rows, rows + 2 * EDGE), -EDGE).astype(jnp.float32).astype(jnp.bfloat16)


def with_edges(before, plane, after):
    has_before, has_after = inside("gy", True), inside("gy", False)
    return jnp.concatenate([before * has_before, plane, after * has_after], axis=0)


def last_kernel(whole, before, after, *sends):
    count = whole.shape[0] // 4
    kernel = row_weights(whole.shape[1])
    me = lax.axis_index("gx")
    for d in range(4):
        quarter = lax.rem(me + d, 4)
        for j in range(count):
            at = count * quarter + j
            sends[d][j] = along_rows(kernel, with_edges(before[at], whole[at], after[at]))


def last_sends(whole, before, after):
    shapes = [(whole.shape[0] // 4,) + whole.shape[1:]] * 4
    return call(last_kernel, shapes, (whole, before, after), 12, 40_000_000)


def rims_kernel(*refs):
    sources, (first, last) = refs[:-2], refs[-2:]
    at = 0
    for source in sources:
        count, rows = source.shape[:2]
        first[at : at + count] = source[:, :EDGE, :]
        last[at : at + count] = source[:, rows - EDGE :, :]
        at += count


def rims(received):
    sources = [array for stage in received for array in stage]
    total = sum(array.shape[0] for array in sources)
    shapes = [(total, EDGE, sources[0].shape[2])] * 2
    return call(rims_kernel, shapes, sources, 12)


def finish_kernel(stage, start, *refs):
    edged, aliased = 0 if start is None else 2, 0 if stage == 0 else 2
    scale, plane_scale, weights, own, up, across, down = refs[:7]
    filtered, projected = refs[7 + edged + aliased : 9 + edged + aliased]
    smooth, sharp, sem = refs[9 + edged + aliased :]
    count, rows, columns = own.shape
    half = columns // 2
    me = lax.axis_index("gx")
    top = jnp.tanh(jnp.float32(sharpness * threshold))
    inverse = 1.0 / (top + jnp.tanh(jnp.float32(sharpness * (1.0 - threshold))))
    sources = [(up, 1), (own, 0), (down, 3), (across, 2)]
    if edged:
        before, after = refs[7:9]
        kernel = row_weights(rows)
    offset = plane_offset(stage, me)
    copies = []
    for j in range(count):
        values = []
        for source, place in sources:
            value = source[j]
            if edged:
                at = start + count * place + j
                value = along_rows(kernel, with_edges(before[at], value, after[at]))
            values.append(value)
        plane_factor = plane_scale[pl.ds(offset + j, 1), :]
        put = pl.ds(j * rows, rows)
        for r in range(4):
            block = lax.rem(me + 3 + r, 4)
            has_before = (block != 0).astype(jnp.float32)
            has_after = (block != 3).astype(jnp.float32)
            outer_values = jnp.where(
                lax.broadcasted_iota(jnp.int32, (rows, half), 1) < half // 2,
                values[(r + 1) % 4][:, :half] * has_after,
                values[(r + 3) % 4][:, half:] * has_before,
            )
            parts = two_parts(values[r]) + two_parts(outer_values)
            summed = jnp.dot(
                jnp.concatenate(parts, axis=1), weights[...], preferred_element_type=jnp.float32
            )
            lanes = pl.ds(pl.multiple_of(block * columns, columns), columns)
            smoothed = summed * (scale[:, lanes] * plane_factor)
            smooth[put, lanes] = smoothed
            sharp[put, lanes] = (
                top + jnp.tanh(sharpness * (smoothed - threshold))
            ) * inverse
        for source, target in ((smooth, filtered), (sharp, projected)):
            copy = pltpu.make_async_copy(
                source.at[put, :], target.at[offset + j], sem.at[len(copies)]
            )
            copy.start()
            copies.append(copy)
    for copy in copies:
        copy.wait()


def finish(stage, tables, received, results, start=None, edges=()):
    scale, plane_scale = tables[:2]
    rows, width = scale.shape
    whole = jax.ShapeDtypeStruct((plane_scale.shape[0], rows, width), jnp.float32)
    count = STAGES[stage]
    args = (*tables, *received, *edges)
    return pl.pallas_call(
        functools.partial(finish_kernel, stage, start),
        out_shape=[whole, whole],
        in_specs=vmem(len(args)) + [pl.BlockSpec(memory_space=pl.ANY)] * len(results),
        out_specs=[pl.BlockSpec(memory_space=pl.ANY)] * 2,
        scratch_shapes=[
            pltpu.VMEM((count * rows, width), jnp.float32),
            pltpu.VMEM((count * rows, width), jnp.float32),
            pltpu.SemaphoreType.DMA((2 * count,)),
        ],
        input_output_aliases={len(args): 0, len(args) + 1: 1} if results else {},
        compiler_params=params(20),
        cost_estimate=cost(40_000_000),
    )(*args, *results)


def one_side(reach):
    return reach * (RADIUS + 1) - reach * (reach + 1) // 2


def edge_sums(position, length):
    reach_left = jnp.minimum(position, RADIUS)
    reach_right = jnp.minimum(length - 1 - position, RADIUS)
    return (RADIUS + 1 + one_side(reach_left) + one_side(reach_right)).astype(jnp.float32)


def scale_kernel(scale, plane_scale, weights):
    rows, width = scale.shape
    layers = plane_scale.shape[0]
    row = lax.axis_index("gy") * rows + lax.broadcasted_iota(jnp.int32, (rows, 128), 0)
    count_y = edge_sums(row, rows * lax.axis_size("gy"))
    for c in range(width // 128):
        column = c * 128 + lax.broadcasted_iota(jnp.int32, (8, 128), 1)
        count_x = edge_sums(column, width)[:1]
        scale[:, c * 128 : (c + 1) * 128] = 1.0 / (count_y * count_x)
    section_place = lax.axis_index("gz") * lax.axis_size("gx") + lax.axis_index("gx")
    plane = section_place * layers + lax.broadcasted_iota(jnp.int32, plane_scale.shape, 0)
    plane_scale[...] = 1.0 / edge_sums(
        plane, layers * lax.axis_size("gx") * lax.axis_size("gz")
    )
    columns = weights.shape[1]
    half = columns // 2
    center = hat((columns, columns), 0)
    row = lax.broadcasted_iota(jnp.int32, (half, columns), 0)
    column = lax.broadcasted_iota(jnp.int32, (half, columns), 1)
    place = jnp.where(row < half // 2, row + columns, row - half)
    outer = jnp.maximum(BOX - jnp.abs(place - column), 0)
    at = 0
    for part in (center, center, outer, outer):
        weights[at : at + part.shape[0], :] = part.astype(jnp.float32).astype(jnp.bfloat16)
        at += part.shape[0]


def scales(rows, width, columns, layers):
    return pl.pallas_call(
        scale_kernel,
        out_shape=[
            jax.ShapeDtypeStruct((rows, width), jnp.float32),
            jax.ShapeDtypeStruct((layers, columns), jnp.float32),
            jax.ShapeDtypeStruct((3 * columns, columns), jnp.bfloat16),
        ],
        out_specs=vmem(3),
        compiler_params=params(4),
        cost_estimate=cost(5_000_000),
        name="scales",
    )()


def shifted(block, axis, distance):
    peers = lax.axis_size(axis)
    route = [(i, (i + distance) % peers) for i in range(peers)]
    return lax.ppermute(block, axis, route)


def around(sends):
    return [sends[0]] + [shifted(sends[d], "gx", d) for d in (1, 2, 3)]


def program(density, mask):
    planes, row_count, columns = density.shape
    groups = lax.axis_size("gx")
    layers = planes // groups
    width = columns * groups
    last = len(STAGES) - 1
    conv, *rest = section(density, mask)
    received = [around(rest[:4])]
    outer = rest[4:]
    halos = []
    for k in range(last):
        halos.append(
            (shifted(outer[2 * k], "gz", 1), shifted(outer[2 * k + 1], "gz", -1))
        )
    tables = scales(row_count, width, columns, layers)
    for stage in range(1, last):
        sends = stage_sends(stage, conv, *halos[stage - 1])
        received.append(around(sends))
    whole, first, final = fill(last, conv, *halos[last - 1])
    before, after = shifted(final, "gy", 1), shifted(first, "gy", -1)
    sends = last_sends(whole, before, after)
    received.append(around(sends))
    results = []
    for group in GROUPS:
        first, final = rims([received[stage] for stage in group])
        ends = (shifted(final, "gy", 1), shifted(first, "gy", -1))
        start = 0
        for stage in group:
            results = finish(stage, tables, received[stage], results, start, ends)
            start += 4 * STAGES[stage]
    results = finish(last, tables, received[last], results)
    return tuple(results)


def solution(mesh):
    placed = (P("gz", "gy", "gx"), P("gz", "gy", "gx"))
    return jax.shard_map(
        program,
        mesh=mesh,
        in_specs=placed,
        out_specs=(P(("gz", "gx"), "gy", None), P(("gz", "gx"), "gy", None)),
        check_vma=False,
    )
```

```python
import functools

import jax
import jax.numpy as jnp
from jax import lax
from jax.experimental import pallas as pl
from jax.experimental.pallas import tpu as pltpu
from jax.sharding import PartitionSpec as P


RADIUS = 6
CELLS = 8
EDGE = 8
BOX = RADIUS + 1

sharpness = 8.0
threshold = 0.5


STAGES = (2, 2, 2, 2)
GROUPS = ((0, 1), (2,))
CHUNKS = 8


def first_of(stage):
    return sum(STAGES[:stage])


def both_offsets(stage):
    ascending = first_of(stage)
    return sum(STAGES) - ascending - STAGES[stage], ascending


def plane_offset(stage, quarter):
    descending, ascending = both_offsets(stage)
    return jnp.where(quarter == 0, descending, ascending)


def outer_places():
    span = 4 * sum(STAGES) + 2 * RADIUS
    places = {}
    for stage in range(1, len(STAGES)):
        first = first_of(stage) - STAGES[0]
        for j in range(STAGES[stage]):
            places[span - first - STAGES[stage] + j] = (stage, 0, j)
            places[first + j] = (stage, 1, j)
    return places


def hat(shape, shift):
    out_index = lax.broadcasted_iota(jnp.int32, shape, 0)
    in_index = lax.broadcasted_iota(jnp.int32, shape, 1)
    distance = jnp.abs(in_index + shift - out_index)
    return jnp.maximum(BOX - distance, 0)


def two_parts(values):
    high = values.astype(jnp.bfloat16)
    low = (values - high.astype(jnp.float32)).astype(jnp.bfloat16)
    return high, low


def along_rows(kernel, values):
    high, low = two_parts(values)
    return jnp.dot(kernel, high, preferred_element_type=jnp.float32) + jnp.dot(
        kernel, low, preferred_element_type=jnp.float32
    )


def vmem(count):
    return [pl.BlockSpec(memory_space=pltpu.VMEM)] * count


def params(mib):
    return pltpu.CompilerParams(vmem_limit_bytes=mib * 1024 * 1024)


def cost(flops):
    return pl.CostEstimate(flops=flops, bytes_accessed=8 * 1024 * 1024, transcendentals=0)


def section_kernel(density, mask, conv, *rest):
    sends, outer = rest[:4], rest[4:-4]
    held, table, codes, sems = rest[-4:]
    places = outer_places()
    planes, rows, columns = density.shape
    blocks = rows // CELLS
    copy_mask = pltpu.make_async_copy(mask, table, sems.at[CHUNKS])
    copy_mask.start()
    copies = []
    for c in range(CHUNKS):
        part = pl.ds(c * (rows // CHUNKS), rows // CHUNKS)
        copies.append(
            pltpu.make_async_copy(density.at[:, part, :], held.at[:, part, :], sems.at[c])
        )
        copies[-1].start()
    spread = (
        lax.broadcasted_iota(jnp.int32, (columns // CELLS, columns), 1) // CELLS
        == lax.broadcasted_iota(jnp.int32, (columns // CELLS, columns), 0)
    )
    copy_mask.wait()
    codes[...] = jnp.dot(
        table[...]
        .reshape(planes // CELLS * blocks, columns // CELLS)
        .astype(jnp.float32)
        .astype(jnp.bfloat16),
        spread.astype(jnp.float32).astype(jnp.bfloat16),
        preferred_element_type=jnp.float32,
    )

    def tile(i, carry):
        row = pl.ds(pl.multiple_of(i * CELLS, CELLS), CELLS)
        values, boxes = [], []
        box = total = None
        for z in range(planes + 2 * RADIUS):
            if z < planes:
                if z % CELLS == 0:
                    code = jnp.broadcast_to(
                        codes[pl.ds(z // CELLS * blocks + i, 1), :], (CELLS, columns)
                    )
                    fixed, given = code < 1.5, jnp.where(code < 0.5, 0.0, 1.0)
                value = jnp.where(fixed, given, held[z, row, :])
                values.append(value)
                change = value - values[z - BOX] if z >= BOX else value
                box = change if box is None else box + change
            elif z < planes + RADIUS:
                box = box - values[z - BOX]
            if z < planes + RADIUS:
                boxes.append(box)
                change = box - boxes[z - BOX] if z >= BOX else box
                total = change if total is None else total + change
            else:
                total = total - boxes[z - BOX]
            if z in places:
                stage, side, j = places[z]
                outer[2 * (stage - 1) + side][j, row, :] = total
            else:
                conv[z - RADIUS, row, :] = total
        return carry

    for c in range(CHUNKS):
        copies[c].wait()
        lax.fori_loop(c * blocks // CHUNKS, (c + 1) * blocks // CHUNKS, tile, 0)
    me = lax.axis_index("gx")
    for distance in range(4):
        quarter = lax.rem(me + distance, 4)
        base = 8 * quarter + plane_offset(0, quarter)
        for j in range(STAGES[0]):
            sends[distance][j] = conv[base + j]


def section(density, mask):
    planes, rows, columns = density.shape
    f32 = functools.partial(jax.ShapeDtypeStruct, dtype=jnp.float32)
    shapes = [f32(density.shape)] + [f32((STAGES[0], rows, columns))] * 4
    for count in STAGES[1:]:
        shapes += [f32((count, rows, columns))] * 2
    return pl.pallas_call(
        section_kernel,
        out_shape=shapes,
        in_specs=[pl.BlockSpec(memory_space=pltpu.HBM)] * 2,
        out_specs=vmem(len(shapes)),
        scratch_shapes=[
            pltpu.VMEM(density.shape, jnp.float32),
            pltpu.VMEM(mask.shape, jnp.int32),
            pltpu.VMEM((planes // CELLS * rows // CELLS, columns), jnp.float32),
            pltpu.SemaphoreType.DMA((CHUNKS + 1,)),
        ],
        compiler_params=params(24),
        cost_estimate=cost(40_000_000),
        name="section",
    )(
        pltpu.with_memory_space_constraint(density, pltpu.HBM),
        pltpu.with_memory_space_constraint(mask, pltpu.HBM),
    )


def inside(axis, first):
    place = lax.axis_index(axis)
    edge = 0 if first else lax.axis_size(axis) - 1
    return (place != edge).astype(jnp.float32)


def call(kernel, shapes, args, mib, flops=20_000_000):
    f32 = [jax.ShapeDtypeStruct(shape, jnp.float32) for shape in shapes]
    return pl.pallas_call(
        kernel,
        out_shape=f32,
        in_specs=vmem(len(args)),
        out_specs=vmem(len(f32)),
        compiler_params=params(mib),
        cost_estimate=cost(flops),
    )(*args)


def stage_kernel(stage, conv, lower, upper, *sends):
    me = lax.axis_index("gx")
    for d in range(4):
        quarter = lax.rem(me + d, 4)
        take_lower = (quarter == 0).astype(jnp.float32) * inside("gz", True)
        take_upper = (quarter == 3).astype(jnp.float32) * inside("gz", False)
        base = 8 * quarter + plane_offset(stage, quarter)
        for j in range(STAGES[stage]):
            sends[d][j] = conv[base + j] + take_lower * lower[j] + take_upper * upper[j]


def stage_sends(stage, conv, lower, upper):
    shapes = [(STAGES[stage],) + conv.shape[1:]] * 4
    kernel = functools.partial(stage_kernel, stage)
    return call(kernel, shapes, (conv, lower, upper), 12)


def fill_kernel(stage, conv, lower, upper, whole, first, last):
    count, rows = STAGES[stage], conv.shape[1]
    for quarter in range(4):
        base = 8 * quarter + both_offsets(stage)[min(quarter, 1)]
        for j in range(count):
            plane = conv[base + j]
            if quarter == 0:
                plane = plane + inside("gz", True) * lower[j]
            if quarter == 3:
                plane = plane + inside("gz", False) * upper[j]
            at = count * quarter + j
            whole[at] = plane
            first[at] = plane[:EDGE]
            last[at] = plane[rows - EDGE :]


def fill(stage, conv, lower, upper):
    total = 4 * STAGES[stage]
    shapes = [(total,) + conv.shape[1:]] + [(total, EDGE, conv.shape[2])] * 2
    kernel = functools.partial(fill_kernel, stage)
    return call(kernel, shapes, (conv, lower, upper), 12)


def row_weights(rows):
    return hat((rows, rows + 2 * EDGE), -EDGE).astype(jnp.float32).astype(jnp.bfloat16)


def with_edges(before, plane, after):
    has_before, has_after = inside("gy", True), inside("gy", False)
    return jnp.concatenate([before * has_before, plane, after * has_after], axis=0)


def last_kernel(whole, before, after, *sends):
    count = whole.shape[0] // 4
    kernel = row_weights(whole.shape[1])
    me = lax.axis_index("gx")
    for d in range(4):
        quarter = lax.rem(me + d, 4)
        for j in range(count):
            at = count * quarter + j
            sends[d][j] = along_rows(kernel, with_edges(before[at], whole[at], after[at]))


def last_sends(whole, before, after):
    shapes = [(whole.shape[0] // 4,) + whole.shape[1:]] * 4
    return call(last_kernel, shapes, (whole, before, after), 12, 40_000_000)


def rims_kernel(*refs):
    sources, (first, last) = refs[:-2], refs[-2:]
    at = 0
    for source in sources:
        count, rows = source.shape[:2]
        first[at : at + count] = source[:, :EDGE, :]
        last[at : at + count] = source[:, rows - EDGE :, :]
        at += count


def rims(received):
    sources = [array for stage in received for array in stage]
    total = sum(array.shape[0] for array in sources)
    shapes = [(total, EDGE, sources[0].shape[2])] * 2
    return call(rims_kernel, shapes, sources, 12)


def finish_kernel(stage, start, *refs):
    edged, aliased = 0 if start is None else 2, 0 if stage == 0 else 2
    scale, plane_scale, weights, own, up, across, down = refs[:7]
    filtered, projected = refs[7 + edged + aliased : 9 + edged + aliased]
    smooth, sharp, sem = refs[9 + edged + aliased :]
    count, rows, columns = own.shape
    half = columns // 2
    me = lax.axis_index("gx")
    top = jnp.tanh(jnp.float32(sharpness * threshold))
    inverse = 1.0 / (top + jnp.tanh(jnp.float32(sharpness * (1.0 - threshold))))
    sources = [(up, 1), (own, 0), (down, 3), (across, 2)]
    if edged:
        before, after = refs[7:9]
        kernel = row_weights(rows)
    offset = plane_offset(stage, me)
    copies = []
    for j in range(count):
        values = []
        for source, place in sources:
            value = source[j]
            if edged:
                at = start + count * place + j
                value = along_rows(kernel, with_edges(before[at], value, after[at]))
            values.append(value)
        plane_factor = plane_scale[pl.ds(offset + j, 1), :]
        put = pl.ds(j * rows, rows)
        for r in range(4):
            block = lax.rem(me + 3 + r, 4)
            has_before = (block != 0).astype(jnp.float32)
            has_after = (block != 3).astype(jnp.float32)
            outer_values = jnp.where(
                lax.broadcasted_iota(jnp.int32, (rows, half), 1) < half // 2,
                values[(r + 1) % 4][:, :half] * has_after,
                values[(r + 3) % 4][:, half:] * has_before,
            )
            parts = two_parts(values[r]) + two_parts(outer_values)
            summed = jnp.dot(
                jnp.concatenate(parts, axis=1), weights[...], preferred_element_type=jnp.float32
            )
            lanes = pl.ds(pl.multiple_of(block * columns, columns), columns)
            smoothed = summed * (scale[:, lanes] * plane_factor)
            smooth[put, lanes] = smoothed
            sharp[put, lanes] = (
                top + jnp.tanh(sharpness * (smoothed - threshold))
            ) * inverse
            for source, target in ((smooth, filtered), (sharp, projected)):
                copy = pltpu.make_async_copy(
                    source.at[put, lanes], target.at[offset + j, :, lanes], sem.at[len(copies)]
                )
                copy.start()
                copies.append(copy)
    for copy in copies:
        copy.wait()


def finish(stage, tables, received, results, start=None, edges=()):
    scale, plane_scale = tables[:2]
    rows, width = scale.shape
    whole = jax.ShapeDtypeStruct((plane_scale.shape[0], rows, width), jnp.float32)
    count = STAGES[stage]
    args = (*tables, *received, *edges)
    return pl.pallas_call(
        functools.partial(finish_kernel, stage, start),
        out_shape=[whole, whole],
        in_specs=vmem(len(args)) + [pl.BlockSpec(memory_space=pl.ANY)] * len(results),
        out_specs=[pl.BlockSpec(memory_space=pl.ANY)] * 2,
        scratch_shapes=[
            pltpu.VMEM((count * rows, width), jnp.float32),
            pltpu.VMEM((count * rows, width), jnp.float32),
            pltpu.SemaphoreType.DMA((8 * count,)),
        ],
        input_output_aliases={len(args): 0, len(args) + 1: 1} if results else {},
        compiler_params=params(20),
        cost_estimate=cost(40_000_000),
    )(*args, *results)


def one_side(reach):
    return reach * (RADIUS + 1) - reach * (reach + 1) // 2


def edge_sums(position, length):
    reach_left = jnp.minimum(position, RADIUS)
    reach_right = jnp.minimum(length - 1 - position, RADIUS)
    return (RADIUS + 1 + one_side(reach_left) + one_side(reach_right)).astype(jnp.float32)


def scale_kernel(scale, plane_scale, weights):
    rows, width = scale.shape
    layers = plane_scale.shape[0]
    row = lax.axis_index("gy") * rows + lax.broadcasted_iota(jnp.int32, (rows, 128), 0)
    count_y = edge_sums(row, rows * lax.axis_size("gy"))
    for c in range(width // 128):
        column = c * 128 + lax.broadcasted_iota(jnp.int32, (8, 128), 1)
        count_x = edge_sums(column, width)[:1]
        scale[:, c * 128 : (c + 1) * 128] = 1.0 / (count_y * count_x)
    section_place = lax.axis_index("gz") * lax.axis_size("gx") + lax.axis_index("gx")
    plane = section_place * layers + lax.broadcasted_iota(jnp.int32, plane_scale.shape, 0)
    plane_scale[...] = 1.0 / edge_sums(
        plane, layers * lax.axis_size("gx") * lax.axis_size("gz")
    )
    columns = weights.shape[1]
    half = columns // 2
    center = hat((columns, columns), 0)
    row = lax.broadcasted_iota(jnp.int32, (half, columns), 0)
    column = lax.broadcasted_iota(jnp.int32, (half, columns), 1)
    place = jnp.where(row < half // 2, row + columns, row - half)
    outer = jnp.maximum(BOX - jnp.abs(place - column), 0)
    at = 0
    for part in (center, center, outer, outer):
        weights[at : at + part.shape[0], :] = part.astype(jnp.float32).astype(jnp.bfloat16)
        at += part.shape[0]


def scales(rows, width, columns, layers):
    return pl.pallas_call(
        scale_kernel,
        out_shape=[
            jax.ShapeDtypeStruct((rows, width), jnp.float32),
            jax.ShapeDtypeStruct((layers, columns), jnp.float32),
            jax.ShapeDtypeStruct((3 * columns, columns), jnp.bfloat16),
        ],
        out_specs=vmem(3),
        compiler_params=params(4),
        cost_estimate=cost(5_000_000),
        name="scales",
    )()


def shifted(block, axis, distance):
    peers = lax.axis_size(axis)
    route = [(i, (i + distance) % peers) for i in range(peers)]
    return lax.ppermute(block, axis, route)


def around(sends):
    return [sends[0]] + [shifted(sends[d], "gx", d) for d in (1, 2, 3)]


def program(density, mask):
    planes, row_count, columns = density.shape
    groups = lax.axis_size("gx")
    layers = planes // groups
    width = columns * groups
    last = len(STAGES) - 1
    conv, *rest = section(density, mask)
    received = [around(rest[:4])]
    outer = rest[4:]
    halos = []
    for k in range(last):
        halos.append((shifted(outer[2 * k], "gz", 1), shifted(outer[2 * k + 1], "gz", -1)))
    tables = scales(row_count, width, columns, layers)
    for stage in range(1, last):
        sends = stage_sends(stage, conv, *halos[stage - 1])
        received.append(around(sends))
    whole, first, final = fill(last, conv, *halos[last - 1])
    before, after = shifted(final, "gy", 1), shifted(first, "gy", -1)
    sends = last_sends(whole, before, after)
    received.append(around(sends))
    results = []
    for group in GROUPS:
        first, final = rims([received[stage] for stage in group])
        ends = (shifted(final, "gy", 1), shifted(first, "gy", -1))
        start = 0
        for stage in group:
            results = finish(stage, tables, received[stage], results, start, ends)
            start += 4 * STAGES[stage]
    results = finish(last, tables, received[last], results)
    return tuple(results)


def solution(mesh):
    placed = (P("gz", "gy", "gx"), P("gz", "gy", "gx"))
    return jax.shard_map(
        program,
        mesh=mesh,
        in_specs=placed,
        out_specs=(P(("gz", "gx"), "gy", None), P(("gz", "gx"), "gy", None)),
        check_vma=False,
    )
```
